256 devices in a mesh: rep: 4 (over x_hi, core), fsdp: 64 (over x_lo, z, y).
Axes of the slice: x: 4 (x_hi: 2, x_lo: 2; x = x_hi * 2 + x_lo), y: 4, z: 8, core: 2. Of those that a mesh axis runs over, the one named last changes fastest.
Arguments:
- layer_inputs: bfloat16 [65536, 4608], P(('rep', 'fsdp')), may hold values from -24 to 24
- queries: bfloat16 [65536, 2048], P(('rep', 'fsdp')), may hold values from -32 to 32
- saved_keys: bfloat16 [65536, 1024], P(('rep', 'fsdp')), may hold values from -6 to 6
- saved_values: bfloat16 [65536, 1024], P(('rep', 'fsdp')), may hold values from -6 to 6
- out_grad: bfloat16 [65536, 2048], P(('rep', 'fsdp')), may hold values from -0.625 to 0.625
- global_params: float32 [4608, 1024], P('fsdp'), may hold values from -0.09375 to 0.09375
- replica_params: float32 [4, 4608, 1024], P('rep', 'fsdp'), may hold values from -0.09375 to 0.09375
- outer_momentum: float32 [4608, 1024], P('fsdp'), may hold values from -0.125 to 0.125
- next_inputs: bfloat16 [65536, 4608], P(('rep', 'fsdp')), may hold values from -6 to 6
Outputs:
- new_params: float32 [4608, 1024], P('fsdp')
- new_momentum: float32 [4608, 1024], P('fsdp')
- next_keys: bfloat16 [65536, 1024], P(('rep', 'fsdp'))
The draws below stay inside these ranges and needn't reach their ends.
All inputs are finite; a program needn't handle non-finite values.
Results may differ from the reference program's by a relative error of at most 0.014.
Values may be sent and summed in bfloat16 or wider, within the bound.
A program may use at most 128 MiB of HBM per device.

```python
import jax
import jax.numpy as jnp
from jax import lax

D = 4608
QH = 16
KVH = 8
HD = 128
SEQ_LEN = 256
TOKENS = 65536
N_REP = 4
N_FSDP = 64


def spiked(array, stream_key, source, target, blocks, factor):
    owner, partner = [(jnp.arange(array.shape[position]) // (array.shape[position] // blocks)).reshape([-1 if axis == position else 1 for axis in range(array.ndim)]) for position in (source, target)]
    chosen = jax.random.permutation(stream_key, blocks)[partner]
    strong = (owner == chosen) | (owner == (partner + blocks // 2) % blocks)
    return jnp.where(strong, factor * array, array)


def shard_levels(rng, dims, shards, low, top_value):
    def one(position, parts):
        heights = jax.random.uniform(jax.random.fold_in(jax.random.fold_in(rng, 6), position), (parts,), jnp.float32, low / len(shards), top_value / len(shards))
        return jnp.repeat(jnp.exp(heights), dims[position] // parts).reshape((-1,) + (1,) * (len(dims) - position - 1))

    factor_of = one(*shards[0])
    for cut in shards[1:]:
        factor_of = factor_of * one(*cut)
    return factor_of


def centred(stream_key, shape, width, reach, cuts=(), dtype=jnp.bfloat16):
    loudness = shard_levels(stream_key, shape, cuts, -0.22, 0.18) if cuts else 1.0
    drawn = jax.random.normal(stream_key, shape, jnp.float32) * width * loudness
    return jnp.minimum(jnp.maximum(drawn, -reach), reach).astype(dtype)


def gaussian_with(rng, extent, deviation, reach, cuts, heavy, kind=jnp.bfloat16):
    drawn = deviation * jax.random.normal(rng, extent, jnp.float32)
    if cuts:
        drawn = drawn * shard_levels(rng, extent, cuts, -0.22, 0.18)
    return jnp.clip(spiked(drawn, jax.random.fold_in(rng, 3), *heavy), -reach, reach).astype(kind)


def setup_inputs(seed: int = 0) -> dict:
    streams_of = jax.random.split(jax.random.key(seed), 10)
    return {
        "layer_inputs": gaussian_with(streams_of[0], (TOKENS, D), 1.0, 24.0, ((0, 256),), (0, 1, 256, 6.0)),
        "queries": centred(streams_of[1], (TOKENS, QH * HD), 5.0, 32.0, ((0, 256),)),
        "saved_keys": centred(streams_of[2], (TOKENS, KVH * HD), 1.0, 6.0, ((0, 256),)),
        "saved_values": centred(streams_of[3], (TOKENS, KVH * HD), 1.0, 6.0, ((0, 256),)),
        "out_grad": centred(streams_of[4], (TOKENS, QH * HD), 0.1, 0.625, ((0, 256),)),
        "global_params": centred(streams_of[5], (D, KVH * HD), D ** -0.5, 0.09375, ((0, 64),), jnp.float32),
        "replica_params": centred(streams_of[6], (N_REP, D, KVH * HD), D ** -0.5, 0.09375, ((0, 4), (1, 64)), jnp.float32),
        "outer_momentum": centred(streams_of[7], (D, KVH * HD), 0.02, 0.125, ((0, 64),), jnp.float32),
        "next_inputs": centred(streams_of[8], (TOKENS, D), 1.0, 6.0, ((0, 256),)),
    }


score_scale = 1.0 / 12.0
soft_cap = 50.0
rope_base = 10000.0
inner_rate = 0.02
outer_rate = 0.7
outer_beta = 0.9


def rotate_back(grads, length):
    half = grads.shape[-1] // 2
    places = jnp.arange(length).astype(jnp.float32)
    freqs = rope_base ** (-jnp.arange(half).astype(jnp.float32) / half)
    angles = (places[:, None] * freqs[None, :])[:, None, :]
    cosine = jnp.cos(angles)
    sine = jnp.sin(angles)
    first = grads[..., :half]
    second = grads[..., half:]
    return jnp.concatenate([first * cosine + second * sine, second * cosine - first * sine], axis=-1)


def attention_keys(query_rows, key_rows, value_rows, grad_rows):
    length = query_rows.shape[0]
    group = QH // KVH
    query_wide = query_rows.astype(jnp.float32).reshape(length, KVH, group, HD)
    key_wide = key_rows.astype(jnp.float32).reshape(length, KVH, HD)
    value_wide = value_rows.astype(jnp.float32).reshape(length, KVH, HD)
    grad_wide = grad_rows.astype(jnp.float32).reshape(length, KVH, group, HD)
    logits = jnp.einsum("ihgd,jhd->hgij", query_wide, key_wide) * score_scale
    capped = jnp.tanh(logits / soft_cap)
    row_index = jnp.arange(length)
    causal = row_index[:, None] >= row_index[None, :]
    unnormed = jnp.where(causal, jnp.exp(soft_cap * capped), jnp.float32(0.0))
    probs = unnormed / jnp.sum(unnormed, axis=-1, keepdims=True)
    dprobs = jnp.einsum("ihgd,jhd->hgij", grad_wide, value_wide)
    center = jnp.sum(probs * dprobs, axis=-1, keepdims=True)
    dlogits = (probs * (dprobs - center) * (1.0 - capped * capped) * score_scale).astype(jnp.bfloat16)
    rotated = jnp.einsum("hgij,ihgd->jhd", dlogits.astype(jnp.float32), query_wide)
    plain = rotate_back(rotated, length)
    return plain.reshape(length, KVH * HD).astype(jnp.bfloat16)


def reference(layer_inputs, queries, saved_keys, saved_values, out_grad, global_params, replica_params, outer_momentum, next_inputs):
    seqs = N_REP * N_FSDP
    packed = (queries.reshape(seqs, SEQ_LEN, QH * HD), saved_keys.reshape(seqs, SEQ_LEN, KVH * HD),
              saved_values.reshape(seqs, SEQ_LEN, KVH * HD), out_grad.reshape(seqs, SEQ_LEN, QH * HD))
    key_grads = lax.map(lambda member: attention_keys(member[0], member[1], member[2], member[3]), packed)
    key_grads = key_grads.reshape(seqs * SEQ_LEN, KVH * HD)
    group_tokens = N_FSDP * SEQ_LEN
    summed = jnp.zeros(global_params.shape, jnp.float32)
    for replica in range(N_REP):
        token_rows = layer_inputs[replica * group_tokens:(replica + 1) * group_tokens]
        grad_rows = key_grads[replica * group_tokens:(replica + 1) * group_tokens]
        group_grad = jnp.dot(token_rows.T, grad_rows, preferred_element_type=jnp.float32)
        finished = replica_params[replica] - inner_rate * group_grad
        summed = summed + (global_params - finished)
    outer_grad = summed / N_REP
    new_momentum = outer_beta * outer_momentum + outer_grad
    new_params = global_params - outer_rate * (outer_grad + outer_beta * new_momentum)
    next_keys = jnp.dot(next_inputs, new_params.astype(jnp.bfloat16), preferred_element_type=jnp.float32).astype(jnp.bfloat16)
    return new_params, new_momentum, next_keys
```

```python
import jax
import jax.numpy as jnp
import numpy as np
from jax import lax
from jax.experimental import pallas as pl
from jax.experimental.pallas import tpu as pltpu
from jax.sharding import PartitionSpec as P

MESH = pl.DeviceIdType.MESH
BF16 = jnp.bfloat16
F32 = jnp.float32

HD = 128
KVH = 8
SEQ = 256
D = 4608
SHARD = 72
THIRD = 24
PORTIONS = 6
STEPS = 7
score_scale = 1.0 / 12.0
soft_cap = 50.0
rope_base = 10000.0
inner_rate = 0.02
outer_rate = 0.7
outer_beta = 0.9

CUBE = ("xa", "ya", "za", "xb", "yb", "zb")


def order_of(k):
    return tuple(CUBE[(k + j) % 6] for j in range(6)) + ("zc",)


def bits_of(x_hi, x_lo, z, y):
    return {
        "xa": (x_hi + x_lo) % 2,
        "xb": x_hi,
        "ya": (y + y // 2) % 2,
        "yb": y // 2,
        "za": (z + z // 2) % 2,
        "zb": (z // 2) % 2,
        "zc": z // 4,
    }


def place_of(bits, k):
    place = 0
    for name in order_of(k):
        place = place * 2 + bits[name]
    return place


def partner_of(name, x_hi, x_lo, z, y):
    if name == "xa":
        return x_hi, 1 - x_lo, z, y
    if name == "xb":
        return 1 - x_hi, 1 - x_lo, z, y
    if name == "ya":
        return x_hi, x_lo, z, y + 1 - 2 * (y % 2)
    if name == "yb":
        return x_hi, x_lo, z, 3 - y
    if name == "za":
        return x_hi, x_lo, z + 1 - 2 * (z % 2), y
    if name == "zb":
        return x_hi, x_lo, (z + 7 + 2 * (z % 2)) % 8, y
    return x_hi, x_lo, (z + 4) % 8, y


def kernel(
    x_ref, q_ref, k_ref, v_ref, g_ref, gp_ref, rp_ref, om_ref, cos_ref, sin_ref, ni_ref,
    np_ref, nm_ref, nk_ref,
    xt, kg, kg_sib, grad, recv, weights, w_full, ni, changes, og, o_send, o_recv,
    rs_send, rs_recv, ag_send, ag_recv, rep_send, rep_recv, og_send, og_recv,
    ni_sem, ni_send, ni_recv, xt_send, xt_recv, kg_send, kg_recv, o_ssem, o_rsem,
):
    rep = lax.axis_index("rep")
    fsdp = lax.axis_index("fsdp")
    x_hi, core = rep // 2, rep % 2
    x_lo, z, y = fsdp // 32, (fsdp // 4) % 8, fsdp % 4

    def device(x_hi, x_lo, z, y, core):
        return (x_hi * 2 + core, (x_lo * 8 + z) * 4 + y)

    sibling = device(x_hi, x_lo, z, y, 1 - core)
    partner = {
        name: device(*partner_of(name, x_hi, x_lo, z, y), core) for name in CUBE + ("zc",)
    }
    rep_peers = [
        (x_hi, 1 - core, sibling),
        (1 - x_hi, core, device(1 - x_hi, x_lo, z, y, core)),
        (1 - x_hi, 1 - core, device(1 - x_hi, x_lo, z, y, 1 - core)),
    ]

    barrier = pltpu.get_barrier_semaphore()
    peers = [sibling] + [partner[name] for name in CUBE + ("zc",)] + [rep_peers[1][2], rep_peers[2][2]]
    for peer in peers:
        pl.semaphore_signal(barrier, inc=1, device_id=peer, device_id_type=MESH)
    pl.semaphore_wait(barrier, len(peers))

    def remote(src, dst, send, receive, peer):
        return pltpu.make_async_remote_copy(
            src_ref=src, dst_ref=dst, send_sem=send, recv_sem=receive, device_id=peer, device_id_type=MESH
        )

    rep_copies = []
    for i, (p_hi, p_core, peer) in enumerate(rep_peers):
        block = pl.ds(pl.multiple_of((p_core * 2 + p_hi) * 256, 256), 256)
        copy = remote(rp_ref.at[:, block], changes.at[i], rep_send.at[i], rep_recv.at[i], peer)
        copy.start()
        rep_copies.append(copy)

    def turn(c, _):
        cols = pl.ds(pl.multiple_of(c * 1152, 1152), 1152)
        xt[pl.ds(pl.multiple_of(c * 1152, 1152), 1152), 0:256] = x_ref[:, cols].T
        return 0

    lax.fori_loop(0, 4, turn, 0)
    xt_copy = remote(xt.at[:, 0:256], xt.at[:, 256:512], xt_send, xt_recv, sibling)
    xt_copy.start()
    ni_local = pltpu.make_async_copy(ni_ref, ni.at[0], ni_sem)
    ni_local.start()
    ni_copy = remote(ni_ref, ni.at[1], ni_send, ni_recv, sibling)
    ni_copy.start()

    nt = (((1,), (1,)), ((), ()))

    def head(h, _):
        lanes = pl.ds(pl.multiple_of(h * HD, HD), HD)
        keys = k_ref[:, lanes]
        values = v_ref[:, lanes]
        low = jnp.zeros((128, HD), F32)
        high = jnp.zeros((128, HD), F32)
        for g in range(2):
            wide = pl.ds(pl.multiple_of(h * 256 + g * HD, HD), HD)
            for b in range(2):
                rows = slice(b * 128, b * 128 + 128)
                n = (b + 1) * 128
                qb = q_ref[rows, wide]
                gb = g_ref[rows, wide]
                logits = lax.dot_general(keys[:n], qb, nt, preferred_element_type=F32)
                dprobs = lax.dot_general(values[:n], gb, nt, preferred_element_type=F32)
                capped = jnp.tanh(logits * (score_scale / soft_cap))
                unnormed = jnp.exp(soft_cap * capped)
                key_at = lax.broadcasted_iota(jnp.int32, (n, 128), 0)
                query_at = lax.broadcasted_iota(jnp.int32, (n, 128), 1) + b * 128
                unnormed = jnp.where(query_at >= key_at, unnormed, 0.0)
                inverse = 1.0 / jnp.sum(unnormed, axis=0, keepdims=True)
                center = jnp.sum(unnormed * dprobs, axis=0, keepdims=True) * inverse
                dlogits = (
                    unnormed * (dprobs - center) * ((1.0 - capped * capped) * (inverse * score_scale))
                ).astype(BF16)
                part = jnp.dot(dlogits, qb, preferred_element_type=F32)
                low = low + part[:128]
                if b == 1:
                    high = high + part[128:]
        half, x_part, ch = h // 4, (h // 2) % 2, h % 2
        out_lanes = pl.ds(pl.multiple_of(x_part * HD, HD), HD)
        for b, rotated in ((0, low), (1, high)):
            rows = slice(b * 128, b * 128 + 128)
            plain = rotated * cos_ref[rows, :] + pltpu.roll(rotated, 64, 1) * sin_ref[rows, :]
            kg[half, ch, rows, out_lanes] = plain.astype(BF16)
        return 0

    lax.fori_loop(0, KVH, head, 0)

    kg_copy = remote(kg.at[1 - core], kg_sib, kg_send, kg_recv, sibling)
    kg_copy.start()
    xt_copy.wait_recv()
    kg_copy.wait_recv()

    mine = bits_of(x_hi, x_lo, z, y)

    def start_of(k, j, flip):
        place = 0
        for name in order_of(k)[:j]:
            place = place * 2 + mine[name]
        last = mine[order_of(k)[j]]
        place = place * 2 + (1 - last if flip else last)
        return place * 2 ** (6 - j)

    def rs_copy(k, j):
        n = 2 ** (6 - j)
        return remote(
            grad.at[k, pl.ds(start_of(k, j, True), n)],
            recv.at[k, pl.ds(128 - 2 * n, n)],
            rs_send.at[k, j],
            rs_recv.at[k, j],
            partner[order_of(k)[j]],
        )

    for ch in range(2):
        def quarter(c, _, ch=ch):
            rows = pl.ds(pl.multiple_of(c * 1152, 1152), 1152)
            part = jnp.dot(
                xt[rows, 0:256], kg[core, ch], preferred_element_type=F32
            ) + jnp.dot(xt[rows, 256:512], kg_sib[ch], preferred_element_type=F32)
            for i in range(16):
                for t_hi in range(2):
                    bits = bits_of(t_hi, c // 2, i // 4, i % 4)
                    bits["zc"] = c % 2
                    for third in range(3):
                        k = ch * 3 + third
                        row = i * SHARD + third * THIRD
                        piece = part[row : row + THIRD, t_hi * 128 : t_hi * 128 + 128]
                        grad[k, place_of(bits, k)] = piece.astype(BF16)
            return 0

        lax.fori_loop(0, 4, quarter, 0)
        for third in range(3):
            rs_copy(ch * 3 + third, 0).start()

    for j in range(STEPS):
        n = 2 ** (6 - j)
        m = min(n, 8)
        for k in range(PORTIONS):
            rs_copy(k, j).wait_recv()
            base = start_of(k, j, False)

            def add(i, _, k=k, n=n, m=m, base=base):
                here = pl.ds(base + i * m, m)
                grad[k, here] = grad[k, here] + recv[k, pl.ds(128 - 2 * n + i * m, m)]
                return 0

            if n == m:
                add(0, 0)
            else:
                lax.fori_loop(0, n // m, add, 0)
            if j + 1 < STEPS:
                rs_copy(k, j + 1).start()

    for copy in rep_copies:
        copy.wait_recv()
    own = core * 2 + x_hi
    for ch in range(2):
        cols = pl.ds(pl.multiple_of(own * 256 + ch * 128, 128), 128)
        lanes = slice(ch * 128, ch * 128 + 128)
        for third in range(3):
            k = ch * 3 + third
            rows = slice(third * THIRD, third * THIRD + THIRD)
            place = start_of(k, 6, False)
            before = gp_ref[rows, cols]
            moved = before - rp_ref[rows, cols]
            for i in range(3):
                moved = moved + (before - changes[i, rows, lanes])
            outer = (moved + inner_rate * grad[k, place].astype(F32)) * 0.25
            og[own, rows, lanes] = outer
            fresh = outer_beta * om_ref[rows, cols] + outer
            weights[k, place] = (before - outer_rate * (outer + outer_beta * fresh)).astype(BF16)

    def ag_copy(k, j):
        n = 2 ** (6 - j)
        here = pl.ds(start_of(k, j, False), n)
        return remote(
            weights.at[k, here], weights.at[k, here], ag_send.at[k, j], ag_recv.at[k, j], partner[order_of(k)[j]]
        )

    for k in range(PORTIONS):
        ag_copy(k, 6).start()
    for j in range(6, 0, -1):
        for k in range(PORTIONS):
            ag_copy(k, j).wait_recv()
            ag_copy(k, j - 1).start()
    og_copies = []
    for i, (_, _, peer) in enumerate(rep_peers):
        copy = remote(og.at[own], og.at[own], og_send.at[i], og_recv.at[i], peer)
        copy.start()
        og_copies.append(copy)
    for k in range(PORTIONS):
        ag_copy(k, 0).wait_recv()

    def place_rows(c, _):
        for i in range(16):
            for t_hi in range(2):
                bits = bits_of(t_hi, c // 2, i // 4, i % 4)
                bits["zc"] = c % 2
                for k in range(PORTIONS):
                    ch, third = k // 3, k % 3
                    row = i * SHARD + third * THIRD
                    lane = t_hi * 256 + ch * 128
                    w_full[c, row : row + THIRD, lane : lane + 128] = weights[k, place_of(bits, k)]
        return 0

    lax.fori_loop(0, 4, place_rows, 0)
    ni_local.wait()
    ni_copy.wait_recv()

    def project(side):
        total = jnp.zeros((SEQ, 512), F32)
        for part in range(2):
            total = total + jnp.dot(
                ni[side, :, part * 2304 : part * 2304 + 2304],
                w_full[2 * part : 2 * part + 2].reshape(2304, 512),
                preferred_element_type=F32,
            )
        return total.astype(BF16)

    o_send[...] = project(1)
    o_copy = remote(o_send, o_recv, o_ssem, o_rsem, sibling)
    o_copy.start()
    nk_ref[:, pl.ds(pl.multiple_of(core * 512, 512), 512)] = project(0)

    for copy in og_copies:
        copy.wait_recv()
    for b in range(4):
        lanes = slice(b * 256, b * 256 + 256)
        outer = og[b]
        fresh = outer_beta * om_ref[:, lanes] + outer
        nm_ref[:, lanes] = fresh
        np_ref[:, lanes] = gp_ref[:, lanes] - outer_rate * (outer + outer_beta * fresh)
    o_copy.wait_recv()
    nk_ref[:, pl.ds(pl.multiple_of((1 - core) * 512, 512), 512)] = o_recv[...]

    for k in range(PORTIONS):
        for j in range(STEPS):
            rs_copy(k, j).wait_send()
            ag_copy(k, j).wait_send()
    for copy in rep_copies + og_copies + [xt_copy, ni_copy, kg_copy, o_copy]:
        copy.wait_send()


def turning():
    half = HD // 2
    freqs = np.float32(rope_base) ** (-np.arange(half, dtype=np.float32) / np.float32(half))
    angles = np.arange(SEQ, dtype=np.float32)[:, None] * freqs[None, :].astype(np.float32)
    cosine, sine = np.cos(angles), np.sin(angles)
    return (
        np.concatenate([cosine, cosine], axis=1).astype(np.float32),
        np.concatenate([sine, -sine], axis=1).astype(np.float32),
    )


def body(layer_inputs, queries, saved_keys, saved_values, out_grad, global_params, replica_params, outer_momentum, next_inputs):
    cosine, sine = turning()
    vmem = pl.BlockSpec(memory_space=pltpu.VMEM)
    dma = pltpu.SemaphoreType.DMA
    return pl.pallas_call(
        kernel,
        out_shape=(
            jax.ShapeDtypeStruct((SHARD, 1024), F32),
            jax.ShapeDtypeStruct((SHARD, 1024), F32),
            jax.ShapeDtypeStruct((SEQ, 1024), BF16),
        ),
        in_specs=[vmem] * 10 + [pl.BlockSpec(memory_space=pl.ANY)],
        out_specs=(vmem, vmem, vmem),
        scratch_shapes=[
            pltpu.VMEM((D, 512), BF16),
            pltpu.VMEM((2, 2, SEQ, 256), BF16),
            pltpu.VMEM((2, SEQ, 256), BF16),
            pltpu.VMEM((PORTIONS, 128, THIRD, 128), BF16),
            pltpu.VMEM((PORTIONS, 128, THIRD, 128), BF16),
            pltpu.VMEM((PORTIONS, 128, THIRD, 128), BF16),
            pltpu.VMEM((4, 1152, 512), BF16),
            pltpu.VMEM((2, SEQ, D), BF16),
            pltpu.VMEM((3, SHARD, 256), F32),
            pltpu.VMEM((4, SHARD, 256), F32),
            pltpu.VMEM((SEQ, 512), BF16),
            pltpu.VMEM((SEQ, 512), BF16),
            dma((PORTIONS, STEPS)),
            dma((PORTIONS, STEPS)),
            dma((PORTIONS, STEPS)),
            dma((PORTIONS, STEPS)),
            dma((3,)),
            dma((3,)),
            dma((3,)),
            dma((3,)),
        ]
        + [dma] * 9,
        compiler_params=pltpu.CompilerParams(
            collective_id=0, has_side_effects=True, vmem_limit_bytes=60 * 1024 * 1024
        ),
    )(
        layer_inputs, queries, saved_keys, saved_values, out_grad, global_params, replica_params[0],
        outer_momentum, cosine, sine, next_inputs,
    )


def solution(mesh):
    both = ("rep", "fsdp")
    return jax.shard_map(
        body,
        mesh=mesh,
        in_specs=(
            P(both, None), P(both, None), P(both, None), P(both, None), P(both, None),
            P("fsdp", None), P("rep", "fsdp", None), P("fsdp", None), P(both, None),
        ),
        out_specs=(P("fsdp", None), P("fsdp", None), P(both, None)),
        check_vma=False,
    )
```

```python
import contextlib

import jax
import jax.numpy as jnp
import numpy as np
from jax import lax
from jax.experimental import pallas as pl
from jax.experimental.pallas import tpu as pltpu
from jax.sharding import PartitionSpec as P

MESH = pl.DeviceIdType.MESH
BF16 = jnp.bfloat16
F32 = jnp.float32

HD = 128
SEQ = 256
D = 4608
SHARD = 72
PORTIONS = 6
SUBS = 3
score_scale = 1.0 / 12.0
soft_cap = 50.0
rope_base = 10000.0
inner_rate = 0.02
outer_rate = 0.7
outer_beta = 0.9

CUBE = ("xa", "ya", "za", "xb", "yb", "zb")


def order_of(k):
    return tuple(CUBE[(k + j) % 6] for j in range(6)) + ("zc",)


def later_z(k):
    return order_of(k).index("zb") < order_of(k).index("za")


def z_bits(hi, lo):
    third = (hi + (lo + 1) // 4) % 2
    return (lo + lo // 2) % 2, (lo // 2 + third) % 2, third


def bits_of(k, x_hi, x_lo, z_hi, z_lo, y):
    bits = {"xa": (x_hi + x_lo) % 2, "xb": x_hi, "ya": (y + y // 2) % 2, "yb": y // 2}
    if later_z(k):
        if isinstance(z_lo, int):
            hi, lo = (z_hi, z_lo - 1) if z_lo else (z_hi + 1, 3)
        else:
            before = (z_hi * 4 + z_lo + 7) % 8
            hi, lo = before // 4, before % 4
        bits["zb"], bits["za"], bits["zc"] = z_bits(hi, lo)
    else:
        bits["za"], bits["zb"], bits["zc"] = z_bits(z_hi, z_lo)
    return bits


def place_of(bits, k):
    place = 0
    for name in order_of(k):
        place = place * 2 + bits[name]
    return place


def partner_of(k, name, x_hi, x_lo, z, y):
    if name == "xa":
        return x_hi, 1 - x_lo, z, y
    if name == "xb":
        return 1 - x_hi, 1 - x_lo, z, y
    if name == "ya":
        return x_hi, x_lo, z, y + 1 - 2 * (y % 2)
    if name == "yb":
        return x_hi, x_lo, z, 3 - y
    if name == "za":
        return x_hi, x_lo, z + 1 - 2 * (z % 2), y
    if name == "zb":
        return x_hi, x_lo, (z + 7 + 2 * (z % 2)) % 8, y
    if later_z(k):
        return x_hi, x_lo, (z + 5 - 2 * (z % 2)) % 8, y
    return x_hi, x_lo, (z + 3 + 2 * (z % 2)) % 8, y


def tile_of(k, s):
    return (s * PORTIONS + k) // 9, (s * PORTIONS + k) % 9


def kernel(
    x_hbm, q_hbm, k_hbm, v_hbm, g_hbm, gp_hbm, rp_hbm, om_hbm, cos_hbm, sin_hbm, ni_hbm,
    np_ref, nm_ref, nk_ref,
    x_ref, q_ref, k_ref, v_ref, g_ref, gp_ref, rp_ref, om_ref, cos_ref, sin_ref, ni,
    xt, kg, kg_sib, grad, recv, n_keep, n_recv, n_sum, n_recv2, n_w, weights, w_full, changes, og, o_send, o_recv,
    in_sem, rs_send, rs_recv, r2_send, r2_recv, keep_send, keep_recv, n_rs_send, n_rs_recv, n_ag_send, n_ag_recv,
    a2_send, a2_recv, own_send, own_recv, ag_send, ag_recv, rep_send, rep_recv, og_send, og_recv,
    ni_send, ni_recv, xt_send, xt_recv, kg_send, kg_recv, o_ssem, o_rsem,
):
    rep = lax.axis_index("rep")
    fsdp = lax.axis_index("fsdp")
    x_hi, core = rep // 2, rep % 2
    x_lo, z, y = fsdp // 32, (fsdp // 4) % 8, fsdp % 4
    portions = range(PORTIONS)

    def device(x_hi, x_lo, z, y, core):
        return (x_hi * 2 + core, (x_lo * 8 + z) * 4 + y)

    def partner(k, j, core):
        return device(*partner_of(k, order_of(k)[j], x_hi, x_lo, z, y), core)

    sibling = device(x_hi, x_lo, z, y, 1 - core)
    across = [device(1 - x_hi, x_lo, z, y, c) for c in range(2)]

    stack = contextlib.ExitStack()

    def phase(name):
        stack.close()
        stack.enter_context(jax.named_scope(name))

    phase("start")
    barrier = pltpu.get_barrier_semaphore()
    peers = [sibling] + across
    for j in range(6):
        peers += [partner(0, j, 0), partner(0, j, 1)]
    peers += [partner(0, 6, core), partner(3, 6, core)]
    for peer in peers:
        pl.semaphore_signal(barrier, inc=1, device_id=peer, device_id_type=MESH)

    loads = [
        pltpu.make_async_copy(src, dst, in_sem.at[i])
        for i, (src, dst) in enumerate(
            (
                (x_hbm, x_ref), (k_hbm, k_ref), (q_hbm, q_ref), (v_hbm, v_ref), (g_hbm, g_ref), (cos_hbm, cos_ref),
                (sin_hbm, sin_ref), (rp_hbm, rp_ref), (gp_hbm, gp_ref), (om_hbm, om_ref), (ni_hbm, ni.at[0]),
            )
        )
    ]
    for load in loads:
        load.start()

    def remote(src, dst, send, receive, peer):
        return pltpu.make_async_remote_copy(
            src_ref=src, dst_ref=dst, send_sem=send, recv_sem=receive, device_id=peer, device_id_type=MESH
        )

    loads[0].wait()

    phase("turn")
    def turn(c, _):
        here = pl.ds(pl.multiple_of(c * 1152, 1152), 1152)
        xt[here, 0:256] = x_ref[:, here].T
        return 0

    lax.fori_loop(0, 4, turn, 0)

    nt = (((1,), (1,)), ((), ()))

    def heads(ch):
        def head(at, _):
            half, x_part = at // 2, at % 2
            h = half * 4 + x_part * 2 + ch
            lanes = pl.ds(pl.multiple_of(h * HD, HD), HD)
            keys = k_ref[:, lanes]
            values = v_ref[:, lanes]
            low = jnp.zeros((128, HD), F32)
            high = jnp.zeros((128, HD), F32)
            for g in range(2):
                wide = pl.ds(pl.multiple_of(h * 256 + g * HD, HD), HD)
                for b in range(2):
                    rows = slice(b * 128, b * 128 + 128)
                    n = (b + 1) * 128
                    qb = q_ref[rows, wide]
                    gb = g_ref[rows, wide]
                    logits = lax.dot_general(keys[:n], qb, nt, preferred_element_type=F32)
                    dprobs = lax.dot_general(values[:n], gb, nt, preferred_element_type=F32)
                    capped = jnp.tanh(logits * (score_scale / soft_cap))
                    unnormed = jnp.exp(soft_cap * capped)
                    key_at = lax.broadcasted_iota(jnp.int32, (n, 128), 0)
                    query_at = lax.broadcasted_iota(jnp.int32, (n, 128), 1) + b * 128
                    unnormed = jnp.where(query_at >= key_at, unnormed, 0.0)
                    inverse = 1.0 / jnp.sum(unnormed, axis=0, keepdims=True)
                    center = jnp.sum(unnormed * dprobs, axis=0, keepdims=True) * inverse
                    dlogits = (
                        unnormed * (dprobs - center) * ((1.0 - capped * capped) * (inverse * score_scale))
                    ).astype(BF16)
                    part = jnp.dot(dlogits, qb, preferred_element_type=F32)
                    low = low + part[:128]
                    if b == 1:
                        high = high + part[128:]
            out_lanes = pl.ds(pl.multiple_of(x_part * HD, HD), HD)
            for b, rotated in ((0, low), (1, high)):
                rows = slice(b * 128, b * 128 + 128)
                plain = rotated * cos_ref[rows, :] + pltpu.roll(rotated, 64, 1) * sin_ref[rows, :]
                kg[half, ch, rows, out_lanes] = plain.astype(BF16)
            return 0

        return head

    def kg_copy(ch):
        return remote(kg.at[1 - core, ch], kg_sib.at[ch], kg_send.at[ch], kg_recv.at[ch], sibling)

    for load in loads[1:8]:
        load.wait()
    phase("attn0")
    lax.fori_loop(0, 2, heads(0), 0)

    phase("barrier")
    pl.semaphore_wait(barrier, len(peers))
    xt_copy = remote(xt.at[:, 0:256], xt.at[:, 256:512], xt_send, xt_recv, sibling)
    xt_copy.start()

    def rep_copy(i, c, slot):
        block = pl.ds(pl.multiple_of(c * 512 + (x_hi if i == 0 else 1 - x_hi) * 256, 256), 256)
        peer = device(x_hi if i == 0 else 1 - x_hi, x_lo, z, y, 1)
        return remote(rp_ref.at[:, block], changes.at[slot, c], rep_send.at[i, c], rep_recv.at[slot, c], peer)

    @pl.when(core == 0)
    def _():
        for c in range(2):
            rep_copy(0, c, 0).start()
            rep_copy(1, c, 2).start()

    @pl.when(core == 1)
    def _():
        for c in range(2):
            rep_copy(1, c, 1).start()

    phase("attn1")
    lax.fori_loop(2, 4, heads(0), 0)
    kg_copy(0).start()
    lax.fori_loop(0, 4, heads(1), 0)
    kg_copy(1).start()
    ni_copy = remote(ni_hbm, ni.at[1], ni_send, ni_recv, sibling)
    ni_copy.start()

    z_hi, z_lo = z // 4, z % 4
    mine = [bits_of(k, x_hi, x_lo, z_hi, z_lo, y) for k in portions]

    def start_of(k, j, flip=False):
        place = 0
        for name in order_of(k)[:j]:
            place = place * 2 + mine[k][name]
        last = mine[k][order_of(k)[j]]
        place = place * 2 + (1 - last if flip else last)
        return place * 2 ** (6 - j)

    def rows_of(s):
        return pl.ds(s * 8, 8)

    def rs_copy(k, j, s):
        n = 2 ** (6 - j)
        return remote(
            grad.at[k, pl.ds(start_of(k, j, True), n), rows_of(s)],
            recv.at[k, pl.ds(128 - 2 * n, n), rows_of(s)],
            rs_send.at[k, j, s],
            rs_recv.at[k, j, s],
            partner(k, j, core),
        )

    def r2_copy(k, s, c):
        return remote(
            grad.at[k, pl.ds(start_of(k, 2, True), 16), rows_of(s)],
            n_recv.at[k, c, :, rows_of(s)],
            r2_send.at[k, s],
            r2_recv.at[c, k, s],
            partner(k, 2, 1),
        )

    def keep_copy(k, s):
        return remote(
            grad.at[k, pl.ds(start_of(k, 2), 16), rows_of(s)],
            n_keep.at[k, :, rows_of(s)],
            keep_send.at[k, s],
            keep_recv.at[k, s],
            sibling,
        )

    for ch in range(2):
        phase(f"grad{ch}")
        if ch == 0:
            xt_copy.wait_recv()
        kg_copy(ch).wait_recv()

        def quarter(c, _, ch=ch):
            rows = pl.ds(pl.multiple_of(c * 1152, 1152), 1152)
            part = jnp.dot(xt[rows, 0:256], kg[core, ch], preferred_element_type=F32) + jnp.dot(
                xt[rows, 256:512], kg_sib[ch], preferred_element_type=F32
            )
            for i in range(16):
                for t_hi in range(2):
                    for k in portions:
                        place = place_of(bits_of(k, t_hi, c // 2, c % 2, i // 4, i % 4), k)
                        for s in range(SUBS):
                            if tile_of(k, s)[0] == ch:
                                row = i * SHARD + tile_of(k, s)[1] * 8
                                piece = part[row : row + 8, t_hi * 128 : t_hi * 128 + 128]
                                grad[k, place, s * 8 : s * 8 + 8] = piece.astype(BF16)
            return 0

        lax.fori_loop(0, 4, quarter, 0)
        for s in range(SUBS):
            for k in portions:
                if tile_of(k, s)[0] == ch:
                    rs_copy(k, 0, s).start()

    for j in range(2):
        n = 2 ** (6 - j)
        for s in range(SUBS):
            phase(f"rs{j}{s}")
            for k in portions:
                rs_copy(k, j, s).wait_recv()
                base = start_of(k, j)

                def add(i, _, k=k, n=n, base=base, s=s):
                    here = pl.ds(base + i * 16, 16)
                    got = recv[k, pl.ds(128 - 2 * n + i * 16, 16), s * 8 : s * 8 + 8]
                    grad[k, here, s * 8 : s * 8 + 8] = grad[k, here, s * 8 : s * 8 + 8] + got
                    return 0

                lax.fori_loop(0, n // 16, add, 0)
                if j == 0:
                    rs_copy(k, 1, s).start()
                else:
                    r2_copy(k, s, core).start()

                    @pl.when(core == 0)
                    def _(k=k, s=s):
                        keep_copy(k, s).start()

    def n_rs_copy(k, j):
        n = 2 ** (6 - j)
        return remote(
            n_sum.at[k, pl.ds(start_of(k, j, True) % 16, n)],
            n_recv2.at[k, pl.ds(16 - 2 * n, n)],
            n_rs_send.at[k, j - 3],
            n_rs_recv.at[k, j - 3],
            partner(k, j, 1),
        )

    def n_ag_copy(k, j):
        n = 2 ** (6 - j)
        here = pl.ds(start_of(k, j) % 16, n)
        return remote(
            n_w.at[k, here], n_w.at[k, here], n_ag_send.at[k, j - 3], n_ag_recv.at[k, j - 3], partner(k, j, 1)
        )

    def a2_copy(k, s, c):
        return remote(
            n_w.at[k, :, c, rows_of(s)],
            weights.at[k, pl.ds(start_of(k, 2), 16), rows_of(s)],
            a2_send.at[c, k, s],
            a2_recv.at[k, s],
            partner(k, 2, c),
        )

    def own_copy(k):
        return remote(
            n_w.at[k, :, 0],
            weights.at[k, pl.ds(start_of(k, 2), 16)],
            own_send.at[k],
            own_recv.at[k],
            sibling,
        )

    def og_copy(i):
        peer = (sibling, across[1], across[0])[i]
        return remote(og.at[x_hi], og.at[x_hi], og_send.at[i], og_recv.at[min(i, 1)], peer)

    @pl.when(core == 1)
    def _():
        for s in range(SUBS):
            phase(f"rs2{s}")
            for k in portions:
                rows = slice(s * 8, s * 8 + 8)
                r2_copy(k, s, 1).wait_recv()
                n_sum[k, :, 1, rows] = grad[k, pl.ds(start_of(k, 2), 16), rows] + n_recv[k, 1, :, rows]
                keep_copy(k, s).wait_recv()
                r2_copy(k, s, 0).wait_recv()
                n_sum[k, :, 0, rows] = n_keep[k, :, rows] + n_recv[k, 0, :, rows]
                if s == SUBS - 1:
                    n_rs_copy(k, 3).start()
        for j in range(3, 7):
            phase(f"rs{j}")
            n = 2 ** (6 - j)
            for k in portions:
                n_rs_copy(k, j).wait_recv()
                here = pl.ds(start_of(k, j) % 16, n)
                n_sum[k, here] = n_sum[k, here] + n_recv2[k, 16 - 2 * n : 16 - n]
                if j < 6:
                    n_rs_copy(k, j + 1).start()

        phase("update")
        for load in loads[8:10]:
            load.wait()
        for c in range(2):
            for slot in range(3):
                rep_copy(1, c, slot).wait_recv()
        for k in portions:
            place = start_of(k, 6) % 16
            for s in range(SUBS):
                ch, tile = tile_of(k, s)
                rows = slice(tile * 8, tile * 8 + 8)
                lanes = slice(ch * 128, ch * 128 + 128)
                for c in range(2):
                    cols = pl.ds(pl.multiple_of(c * 512 + x_hi * 256 + ch * 128, 128), 128)
                    before = gp_ref[rows, cols]
                    moved = before - rp_ref[rows, cols]
                    for slot in range(3):
                        moved = moved + (before - changes[slot, c, rows, lanes])
                    summed = n_sum[k, place, c, s * 8 : s * 8 + 8].astype(F32)
                    outer = (moved + inner_rate * summed) * 0.25
                    og[x_hi, c, rows, lanes] = outer
                    fresh = outer_beta * om_ref[rows, cols] + outer
                    n_w[k, place, c, s * 8 : s * 8 + 8] = (
                        before - outer_rate * (outer + outer_beta * fresh)
                    ).astype(BF16)
            n_ag_copy(k, 6).start()
        for i in range(3):
            og_copy(i).start()
        for j in range(6, 2, -1):
            phase(f"ag{j}")
            for k in portions:
                n_ag_copy(k, j).wait_recv()
                if j > 3:
                    n_ag_copy(k, j - 1).start()
                else:
                    own_copy(k).start()
                    for s in range(SUBS):
                        for c in range(2):
                            a2_copy(k, s, c).start()
        for k in portions:
            weights[k, pl.ds(start_of(k, 2), 16)] = n_w[k, :, 1]

    @pl.when(core == 0)
    def _():
        phase("agown")
        for load in loads[8:10]:
            load.wait()
        for k in portions:
            own_copy(k).wait_recv()

    def ag_copy(k, j, s):
        here = pl.ds(start_of(k, j), 2 ** (6 - j))
        return remote(
            weights.at[k, here, rows_of(s)],
            weights.at[k, here, rows_of(s)],
            ag_send.at[k, j, s],
            ag_recv.at[k, j, s],
            partner(k, j, core),
        )

    for s in range(SUBS):
        phase(f"ag2{s}")
        for k in portions:
            a2_copy(k, s, 0).wait_recv()
            ag_copy(k, 1, s).start()
    for s in range(SUBS):
        phase(f"ag1{s}")
        for k in portions:
            ag_copy(k, 1, s).wait_recv()
            ag_copy(k, 0, s).start()

    def o_copy(ch):
        return remote(o_send.at[ch], o_recv.at[ch], o_ssem.at[ch], o_rsem.at[ch], sibling)

    def project(side, ch):
        total = jnp.zeros((SEQ, 256), F32)
        for part in range(2):
            total = total + jnp.dot(
                ni[side, :, part * 2304 : part * 2304 + 2304],
                w_full[2 * part : 2 * part + 2].reshape(2304, 256),
                preferred_element_type=F32,
            )
        return total.astype(BF16)

    def to_output(half, ch, block):
        for t_hi in range(2):
            lanes = pl.ds(pl.multiple_of(half * 512 + t_hi * 256 + ch * 128, 128), 128)
            nk_ref[:, lanes] = block[:, t_hi * 128 : t_hi * 128 + 128]

    for ch in range(2):
        phase(f"ag0{ch}")
        for s in range(SUBS):
            for k in portions:
                if tile_of(k, s)[0] == ch:
                    ag_copy(k, 0, s).wait_recv()

        phase(f"place{ch}")
        def place_rows(c, _, ch=ch):
            for i in range(16):
                for t_hi in range(2):
                    for k in portions:
                        place = place_of(bits_of(k, t_hi, c // 2, c % 2, i // 4, i % 4), k)
                        for s in range(SUBS):
                            if tile_of(k, s)[0] == ch:
                                row = i * SHARD + tile_of(k, s)[1] * 8
                                w_full[c, row : row + 8, t_hi * 128 : t_hi * 128 + 128] = weights[
                                    k, place, s * 8 : s * 8 + 8
                                ]
            return 0

        lax.fori_loop(0, 4, place_rows, 0)
        if ch == 0:
            loads[10].wait()
            ni_copy.wait_recv()
        phase(f"proj{ch}")
        o_send[ch] = project(1, ch)
        o_copy(ch).start()
        to_output(core, ch, project(0, ch))

    phase("tail")
    @pl.when(core == 0)
    def _():
        og_copy(0).wait_recv()

    og_copy(1).wait_recv()
    for b in range(4):
        lanes = slice(b * 256, b * 256 + 256)
        outer = og[b % 2, b // 2]
        fresh = outer_beta * om_ref[:, lanes] + outer
        nm_ref[:, lanes] = fresh
        np_ref[:, lanes] = gp_ref[:, lanes] - outer_rate * (outer + outer_beta * fresh)
    phase("owait")
    for ch in range(2):
        o_copy(ch).wait_recv()
        to_output(1 - core, ch, o_recv[ch])

    phase("sends")
    for s in range(SUBS):
        for k in portions:
            for j in range(2):
                rs_copy(k, j, s).wait_send()
                ag_copy(k, j, s).wait_send()
            r2_copy(k, s, 0).wait_send()
    for ch in range(2):
        kg_copy(ch).wait_send()
        o_copy(ch).wait_send()
    xt_copy.wait_send()
    ni_copy.wait_send()
    for c in range(2):
        rep_copy(1, c, 0).wait_send()

    @pl.when(core == 0)
    def _():
        for c in range(2):
            rep_copy(0, c, 0).wait_send()
        for k in portions:
            for s in range(SUBS):
                keep_copy(k, s).wait_send()

    @pl.when(core == 1)
    def _():
        for i in range(3):
            og_copy(i).wait_send()
        for k in portions:
            own_copy(k).wait_send()
            for j in range(3, 7):
                n_rs_copy(k, j).wait_send()
                n_ag_copy(k, j).wait_send()
            for s in range(SUBS):
                for c in range(2):
                    a2_copy(k, s, c).wait_send()
    stack.close()


def turning():
    half = HD // 2
    freqs = np.float32(rope_base) ** (-np.arange(half, dtype=np.float32) / np.float32(half))
    angles = np.arange(SEQ, dtype=np.float32)[:, None] * freqs[None, :].astype(np.float32)
    cosine, sine = np.cos(angles), np.sin(angles)
    return (
        np.concatenate([cosine, cosine], axis=1).astype(np.float32),
        np.concatenate([sine, -sine], axis=1).astype(np.float32),
    )


def body(layer_inputs, queries, saved_keys, saved_values, out_grad, global_params, replica_params, outer_momentum, next_inputs):
    cosine, sine = turning()
    vmem = pl.BlockSpec(memory_space=pltpu.VMEM)
    dma = pltpu.SemaphoreType.DMA
    rows = pltpu.VMEM((SHARD, 1024), F32)
    table = pltpu.VMEM((SEQ, HD), F32)
    return pl.pallas_call(
        kernel,
        out_shape=(
            jax.ShapeDtypeStruct((SHARD, 1024), F32),
            jax.ShapeDtypeStruct((SHARD, 1024), F32),
            jax.ShapeDtypeStruct((SEQ, 1024), BF16),
        ),
        in_specs=[pl.BlockSpec(memory_space=pl.ANY)] * 11,
        out_specs=(vmem, vmem, vmem),
        scratch_shapes=[
            pltpu.VMEM((SEQ, D), BF16),
            pltpu.VMEM((SEQ, 2048), BF16),
            pltpu.VMEM((SEQ, 1024), BF16),
            pltpu.VMEM((SEQ, 1024), BF16),
            pltpu.VMEM((SEQ, 2048), BF16),
            rows, rows, rows, table, table,
            pltpu.VMEM((2, SEQ, D), BF16),
            pltpu.VMEM((D, 512), BF16),
            pltpu.VMEM((2, 2, SEQ, 256), BF16),
            pltpu.VMEM((2, SEQ, 256), BF16),
            pltpu.VMEM((PORTIONS, 128, 24, 128), BF16),
            pltpu.VMEM((PORTIONS, 96, 24, 128), BF16),
            pltpu.VMEM((PORTIONS, 16, 24, 128), BF16),
            pltpu.VMEM((PORTIONS, 2, 16, 24, 128), BF16),
            pltpu.VMEM((PORTIONS, 16, 2, 24, 128), BF16),
            pltpu.VMEM((PORTIONS, 16, 2, 24, 128), BF16),
            pltpu.VMEM((PORTIONS, 16, 2, 24, 128), BF16),
            pltpu.VMEM((PORTIONS, 128, 24, 128), BF16),
            pltpu.VMEM((4, 1152, 256), BF16),
            pltpu.VMEM((3, 2, SHARD, 256), F32),
            pltpu.VMEM((2, 2, SHARD, 256), F32),
            pltpu.VMEM((2, SEQ, 256), BF16),
            pltpu.VMEM((2, SEQ, 256), BF16),
            dma((11,)),
            dma((PORTIONS, 2, SUBS)), dma((PORTIONS, 2, SUBS)),
            dma((PORTIONS, SUBS)), dma((2, PORTIONS, SUBS)),
            dma((PORTIONS, SUBS)), dma((PORTIONS, SUBS)),
            dma((PORTIONS, 4)), dma((PORTIONS, 4)),
            dma((PORTIONS, 4)), dma((PORTIONS, 4)),
            dma((2, PORTIONS, SUBS)), dma((PORTIONS, SUBS)),
            dma((PORTIONS,)), dma((PORTIONS,)),
            dma((PORTIONS, 2, SUBS)), dma((PORTIONS, 2, SUBS)),
            dma((2, 2)), dma((3, 2)),
            dma((3,)), dma((2,)),
            dma, dma, dma, dma, dma((2,)), dma((2,)), dma((2,)), dma((2,)),
        ],
        compiler_params=pltpu.CompilerParams(
            collective_id=0, has_side_effects=True, vmem_limit_bytes=60 * 1024 * 1024
        ),
    )(
        layer_inputs, queries, saved_keys, saved_values, out_grad, global_params, replica_params[0],
        outer_momentum, cosine, sine, next_inputs,
    )


def solution(mesh):
    both = ("rep", "fsdp")
    return jax.shard_map(
        body,
        mesh=mesh,
        in_specs=(
            P(both, None), P(both, None), P(both, None), P(both, None), P(both, None),
            P("fsdp", None), P("rep", "fsdp", None), P("fsdp", None), P(both, None),
        ),
        out_specs=(P("fsdp", None), P("fsdp", None), P(both, None)),
        check_vma=False,
    )
```

```python
import contextlib

import jax
import jax.numpy as jnp
import numpy as np
from jax import lax
from jax.experimental import pallas as pl
from jax.experimental.pallas import tpu as pltpu
from jax.sharding import PartitionSpec as P

MESH = pl.DeviceIdType.MESH
BF16 = jnp.bfloat16
F32 = jnp.float32

HD = 128
SEQ = 256
D = 4608
SHARD = 72
PORTIONS = 6
SUBS = 3
score_scale = 1.0 / 12.0
soft_cap = 50.0
rope_base = 10000.0
inner_rate = 0.02
outer_rate = 0.7
outer_beta = 0.9

CUBE = ("xa", "ya", "za", "xb", "yb", "zb")


def order_of(k):
    return tuple(CUBE[(k + j) % 6] for j in range(6)) + ("zc",)


def later_z(k):
    return order_of(k).index("zb") < order_of(k).index("za")


def z_bits(hi, lo):
    third = (hi + (lo + 1) // 4) % 2
    return (lo + lo // 2) % 2, (lo // 2 + third) % 2, third


def bits_of(k, x_hi, x_lo, z_hi, z_lo, y):
    bits = {"xa": (x_hi + x_lo) % 2, "xb": x_hi, "ya": (y + y // 2) % 2, "yb": y // 2}
    if later_z(k):
        if isinstance(z_lo, int):
            hi, lo = (z_hi, z_lo - 1) if z_lo else (z_hi + 1, 3)
        else:
            before = (z_hi * 4 + z_lo + 7) % 8
            hi, lo = before // 4, before % 4
        bits["zb"], bits["za"], bits["zc"] = z_bits(hi, lo)
    else:
        bits["za"], bits["zb"], bits["zc"] = z_bits(z_hi, z_lo)
    return bits


def place_of(bits, k):
    place = 0
    for name in order_of(k):
        place = place * 2 + bits[name]
    return place


def partner_of(k, name, x_hi, x_lo, z, y):
    if name == "xa":
        return x_hi, 1 - x_lo, z, y
    if name == "xb":
        return 1 - x_hi, 1 - x_lo, z, y
    if name == "ya":
        return x_hi, x_lo, z, y + 1 - 2 * (y % 2)
    if name == "yb":
        return x_hi, x_lo, z, 3 - y
    if name == "za":
        return x_hi, x_lo, z + 1 - 2 * (z % 2), y
    if name == "zb":
        return x_hi, x_lo, (z + 7 + 2 * (z % 2)) % 8, y
    if later_z(k):
        return x_hi, x_lo, (z + 5 - 2 * (z % 2)) % 8, y
    return x_hi, x_lo, (z + 3 + 2 * (z % 2)) % 8, y


def tile_of(k, s):
    return (s * PORTIONS + k) // 9, (s * PORTIONS + k) % 9


def kernel(
    x_hbm, q_hbm, k_hbm, v_hbm, g_hbm, gp_hbm, rp_hbm, om_hbm, cos_hbm, sin_hbm, ni_hbm,
    np_ref, nm_ref, nk_ref,
    x_ref, q_ref, k_ref, v_ref, g_ref, gp_ref, rp_ref, om_ref, cos_ref, sin_ref, ni,
    xt, kg, kg_sib, grad, recv, n_keep, n_recv, n_sum, n_recv2, n_w, weights, w_full, changes, og, o_send, o_recv, anchor,
    in_sem, rs_send, rs_recv, r2_send, r2_recv, keep_send, keep_recv, n_rs_send, n_rs_recv, n_ag_send, n_ag_recv,
    a2_send, a2_recv, own_send, own_recv, ag_send, ag_recv, rep_send, rep_recv, og_send, og_recv, base_send, base_recv,
    ni_send, ni_recv, xt_send, xt_recv, kg_send, kg_recv, o_ssem, o_rsem,
):
    rep = lax.axis_index("rep")
    fsdp = lax.axis_index("fsdp")
    x_hi, core = rep // 2, rep % 2
    x_lo, z, y = fsdp // 32, (fsdp // 4) % 8, fsdp % 4
    portions = range(PORTIONS)

    def device(x_hi, x_lo, z, y, core):
        return (x_hi * 2 + core, (x_lo * 8 + z) * 4 + y)

    def partner(k, j, core):
        return device(*partner_of(k, order_of(k)[j], x_hi, x_lo, z, y), core)

    def corner(k):
        return partner_of(k, order_of(k)[4], *partner_of(k, order_of(k)[3], x_hi, x_lo, z, y))

    def both_of(k, core):
        return device(*corner(k), core)

    sibling = device(x_hi, x_lo, z, y, 1 - core)
    across = [device(1 - x_hi, x_lo, z, y, c) for c in range(2)]

    stack = contextlib.ExitStack()

    def phase(name):
        stack.close()
        stack.enter_context(jax.named_scope(name))

    phase("start")
    barrier = pltpu.get_barrier_semaphore()
    peers = [sibling] + across
    for j in range(6):
        peers += [partner(0, j, 0), partner(0, j, 1)]
    peers += [partner(0, 6, core), partner(3, 6, core)] + [both_of(k, core) for k in portions]
    for peer in peers:
        pl.semaphore_signal(barrier, inc=1, device_id=peer, device_id_type=MESH)

    loads = [
        pltpu.make_async_copy(src, dst, in_sem.at[i])
        for i, (src, dst) in enumerate(
            (
                (x_hbm, x_ref), (k_hbm, k_ref), (q_hbm, q_ref), (v_hbm, v_ref), (g_hbm, g_ref), (cos_hbm, cos_ref),
                (sin_hbm, sin_ref), (rp_hbm, rp_ref), (gp_hbm, gp_ref), (om_hbm, om_ref), (ni_hbm, ni.at[0]),
            )
        )
    ]
    for load in loads:
        load.start()

    def remote(src, dst, send, receive, peer):
        return pltpu.make_async_remote_copy(
            src_ref=src, dst_ref=dst, send_sem=send, recv_sem=receive, device_id=peer, device_id_type=MESH
        )

    loads[0].wait()

    phase("turn")
    def turn(c, _):
        here = pl.ds(pl.multiple_of(c * 1152, 1152), 1152)
        xt[here, 0:256] = x_ref[:, here].T
        return 0

    lax.fori_loop(0, 4, turn, 0)

    nt = (((1,), (1,)), ((), ()))

    def heads(ch):
        def head(at, _):
            half, x_part = at // 2, at % 2
            h = half * 4 + x_part * 2 + ch
            lanes = pl.ds(pl.multiple_of(h * HD, HD), HD)
            keys = k_ref[:, lanes]
            values = v_ref[:, lanes]
            low = jnp.zeros((128, HD), F32)
            high = jnp.zeros((128, HD), F32)
            for g in range(2):
                wide = pl.ds(pl.multiple_of(h * 256 + g * HD, HD), HD)
                for b in range(2):
                    rows = slice(b * 128, b * 128 + 128)
                    n = (b + 1) * 128
                    qb = q_ref[rows, wide]
                    gb = g_ref[rows, wide]
                    logits = lax.dot_general(keys[:n], qb, nt, preferred_element_type=F32)
                    dprobs = lax.dot_general(values[:n], gb, nt, preferred_element_type=F32)
                    capped = jnp.tanh(logits * (score_scale / soft_cap))
                    unnormed = jnp.exp(soft_cap * capped)
                    key_at = lax.broadcasted_iota(jnp.int32, (n, 128), 0)
                    query_at = lax.broadcasted_iota(jnp.int32, (n, 128), 1) + b * 128
                    unnormed = jnp.where(query_at >= key_at, unnormed, 0.0)
                    inverse = 1.0 / jnp.sum(unnormed, axis=0, keepdims=True)
                    center = jnp.sum(unnormed * dprobs, axis=0, keepdims=True) * inverse
                    dlogits = (
                        unnormed * (dprobs - center) * ((1.0 - capped * capped) * (inverse * score_scale))
                    ).astype(BF16)
                    part = jnp.dot(dlogits, qb, preferred_element_type=F32)
                    low = low + part[:128]
                    if b == 1:
                        high = high + part[128:]
            out_lanes = pl.ds(pl.multiple_of(x_part * HD, HD), HD)
            for b, rotated in ((0, low), (1, high)):
                rows = slice(b * 128, b * 128 + 128)
                plain = rotated * cos_ref[rows, :] + pltpu.roll(rotated, 64, 1) * sin_ref[rows, :]
                kg[half, ch, rows, out_lanes] = plain.astype(BF16)
            return 0

        return head

    def kg_copy(ch):
        return remote(kg.at[1 - core, ch], kg_sib.at[ch], kg_send.at[ch], kg_recv.at[ch], sibling)

    phase("barrier")
    pl.semaphore_wait(barrier, len(peers))
    xt_copy = remote(xt.at[:, 0:256], xt.at[:, 256:512], xt_send, xt_recv, sibling)
    xt_copy.start()

    def rep_copy(i, c, slot):
        block = pl.ds(pl.multiple_of(c * 512 + (x_hi if i == 0 else 1 - x_hi) * 256, 256), 256)
        peer = device(x_hi if i == 0 else 1 - x_hi, x_lo, z, y, 1)
        return remote(rp_ref.at[:, block], changes.at[slot, c], rep_send.at[i, c], rep_recv.at[slot, c], peer)

    loads[7].wait()

    @pl.when(core == 0)
    def _():
        for c in range(2):
            rep_copy(0, c, 0).start()
            rep_copy(1, c, 2).start()

    @pl.when(core == 1)
    def _():
        for c in range(2):
            rep_copy(1, c, 1).start()

    for load in loads[1:7]:
        load.wait()
    phase("attn0")
    lax.fori_loop(0, 4, heads(0), 0)
    kg_copy(0).start()
    phase("attn1a")
    lax.fori_loop(0, 2, heads(1), 0)
    ni_copy = remote(ni_hbm, ni.at[1], ni_send, ni_recv, sibling)

    z_hi, z_lo = z // 4, z % 4
    mine = [bits_of(k, x_hi, x_lo, z_hi, z_lo, y) for k in portions]

    def start_of(k, j, flip=False):
        place = 0
        for name in order_of(k)[:j]:
            place = place * 2 + mine[k][name]
        last = mine[k][order_of(k)[j]]
        place = place * 2 + (1 - last if flip else last)
        return place * 2 ** (6 - j)

    def rows_of(s):
        return pl.ds(s * 8, 8)

    def rs_copy(k, j, s):
        n = 2 ** (6 - j)
        return remote(
            grad.at[k, pl.ds(start_of(k, j, True), n), rows_of(s)],
            recv.at[k, pl.ds(128 - 2 * n, n), rows_of(s)],
            rs_send.at[k, j, s],
            rs_recv.at[k, j, s],
            partner(k, j, core),
        )

    def base_copy(side):
        part = pl.ds(side * 3, 3)
        return remote(anchor.at[0, part], anchor.at[1, part], base_send.at[side], base_recv.at[side], partner(side * 3, 6, 1))

    def make_base():
        for load in loads[8:10]:
            load.wait()
        for c in range(2):
            for slot in range(3):
                rep_copy(1, c, slot).wait_recv()
        for k in portions:
            for s in range(SUBS):
                ch, tile = tile_of(k, s)
                rows = slice(tile * 8, tile * 8 + 8)
                lanes = slice(ch * 128, ch * 128 + 128)
                for c in range(2):
                    cols = pl.ds(pl.multiple_of(c * 512 + x_hi * 256 + ch * 128, 128), 128)
                    before = gp_ref[rows, cols]
                    moved = before - rp_ref[rows, cols]
                    for slot in range(3):
                        moved = moved + (before - changes[slot, c, rows, lanes])
                    outer = moved * 0.25
                    og[x_hi, c, rows, lanes] = outer
                    anchor[0, k, c, s * 8 : s * 8 + 8] = before - outer_rate * (
                        (1.0 + outer_beta) * outer + outer_beta * outer_beta * om_ref[rows, cols]
                    )
        for side in range(2):
            base_copy(side).start()

    def r2_copy(k, s, c):
        return remote(
            grad.at[k, pl.ds(start_of(k, 2, True), 16), rows_of(s)],
            n_recv.at[k, c, :, rows_of(s)],
            r2_send.at[k, s],
            r2_recv.at[c, k, s],
            partner(k, 2, 1),
        )

    def keep_copy(k, s):
        return remote(
            grad.at[k, pl.ds(start_of(k, 2), 16), rows_of(s)],
            n_keep.at[k, :, rows_of(s)],
            keep_send.at[k, s],
            keep_recv.at[k, s],
            sibling,
        )

    for ch in range(2):
        if ch == 0:
            phase("base")

            @pl.when(core == 1)
            def _():
                make_base()

            phase("xtwait")
            xt_copy.wait_recv()
        else:
            phase("attn1b")
            lax.fori_loop(2, 4, heads(1), 0)
            kg_copy(1).start()
            ni_copy.start()
            phase("kgwait")
        kg_copy(ch).wait_recv()
        phase(f"grad{ch}")

        def quarter(c, _, ch=ch):
            rows = pl.ds(pl.multiple_of(c * 1152, 1152), 1152)
            part = jnp.dot(xt[rows, 0:256], kg[core, ch], preferred_element_type=F32) + jnp.dot(
                xt[rows, 256:512], kg_sib[ch], preferred_element_type=F32
            )
            for i in range(16):
                for t_hi in range(2):
                    for k in portions:
                        place = place_of(bits_of(k, t_hi, c // 2, c % 2, i // 4, i % 4), k)
                        for s in range(SUBS):
                            if tile_of(k, s)[0] == ch:
                                row = i * SHARD + tile_of(k, s)[1] * 8
                                piece = part[row : row + 8, t_hi * 128 : t_hi * 128 + 128]
                                grad[k, place, s * 8 : s * 8 + 8] = piece.astype(BF16)
            return 0

        lax.fori_loop(0, 4, quarter, 0)
        for s in range(SUBS):
            for k in portions:
                if tile_of(k, s)[0] == ch:
                    rs_copy(k, 0, s).start()

    for j in range(2):
        n = 2 ** (6 - j)
        for s in range(SUBS):
            phase(f"rs{j}{s}")
            for k in portions:
                rs_copy(k, j, s).wait_recv()
                base = start_of(k, j)

                def add(i, _, k=k, n=n, base=base, s=s):
                    here = pl.ds(base + i * 16, 16)
                    got = recv[k, pl.ds(128 - 2 * n + i * 16, 16), s * 8 : s * 8 + 8]
                    grad[k, here, s * 8 : s * 8 + 8] = grad[k, here, s * 8 : s * 8 + 8] + got
                    return 0

                lax.fori_loop(0, n // 16, add, 0)
                if j == 0:
                    rs_copy(k, 1, s).start()
                else:
                    r2_copy(k, s, core).start()

                    @pl.when(core == 0)
                    def _(k=k, s=s):
                        keep_copy(k, s).start()

    quad = []
    for k in portions:
        at = []
        for chip in (
            partner_of(k, order_of(k)[3], x_hi, x_lo, z, y),
            partner_of(k, order_of(k)[4], x_hi, x_lo, z, y),
            corner(k),
        ):
            there = bits_of(k, chip[0], chip[1], chip[2] // 4, chip[2] % 4, chip[3])
            at.append((device(*chip, 1), (there[order_of(k)[3]] * 2 + there[order_of(k)[4]]) * 4))
        quad.append(at)

    def n_rs4_copy(k, i):
        peer, start = quad[k][i]
        return remote(
            n_sum.at[k, pl.ds(start, 4)],
            n_recv2.at[k, pl.ds(4 * i, 4)],
            n_rs_send.at[k, i],
            n_rs_recv.at[k, i],
            peer,
        )

    def n_ag4_copy(k, i):
        here = pl.ds(start_of(k, 4) % 16, 4)
        return remote(n_w.at[k, here], n_w.at[k, here], n_ag_send.at[k, i], n_ag_recv.at[k, i], quad[k][i][0])

    def n_rs5_copy(k):
        return remote(
            n_sum.at[k, pl.ds(start_of(k, 5, True) % 16, 2)],
            n_recv2.at[k, pl.ds(12, 2)],
            n_rs_send.at[k, 3],
            n_rs_recv.at[k, 3],
            partner(k, 5, 1),
        )

    def n_rs6_copy(k):
        return remote(
            n_sum.at[k, pl.ds(start_of(k, 5) % 16, 2)],
            n_recv2.at[k, pl.ds(14, 2)],
            n_rs_send.at[k, 4],
            n_rs_recv.at[k, 4],
            partner(k, 6, 1),
        )

    def n_ag5_copy(k):
        here = pl.ds(start_of(k, 5) % 16, 2)
        return remote(n_w.at[k, here], n_w.at[k, here], n_ag_send.at[k, 3], n_ag_recv.at[k, 3], partner(k, 5, 1))

    def a2_copy(k, s, c):
        return remote(
            n_w.at[k, :, c, rows_of(s)],
            weights.at[k, pl.ds(start_of(k, 2), 16), rows_of(s)],
            a2_send.at[c, k, s],
            a2_recv.at[k, s],
            partner(k, 2, c),
        )

    def own_copy(k):
        return remote(
            n_w.at[k, :, 0],
            weights.at[k, pl.ds(start_of(k, 2), 16)],
            own_send.at[k],
            own_recv.at[k],
            sibling,
        )

    def og_copy(i):
        peer = (sibling, across[1], across[0])[i]
        return remote(og.at[x_hi], og.at[x_hi], og_send.at[i], og_recv.at[min(i, 1)], peer)

    @pl.when(core == 1)
    def _():
        for s in range(SUBS):
            phase(f"rs2{s}")
            for k in portions:
                rows = slice(s * 8, s * 8 + 8)
                r2_copy(k, s, 1).wait_recv()
                n_sum[k, :, 1, rows] = grad[k, pl.ds(start_of(k, 2), 16), rows] + n_recv[k, 1, :, rows]
                keep_copy(k, s).wait_recv()
                r2_copy(k, s, 0).wait_recv()
                n_sum[k, :, 0, rows] = n_keep[k, :, rows] + n_recv[k, 0, :, rows]
                if s == SUBS - 1:
                    for i in range(3):
                        n_rs4_copy(k, i).start()
        phase("rs34")
        for k in portions:
            for i in range(3):
                n_rs4_copy(k, i).wait_recv()
            here = pl.ds(start_of(k, 4) % 16, 4)
            total = n_sum[k, here].astype(F32)
            for i in range(3):
                total = total + n_recv2[k, 4 * i : 4 * i + 4].astype(F32)
            n_sum[k, here] = total.astype(BF16)
            n_rs5_copy(k).start()
        phase("rs5")
        for k in portions:
            n_rs5_copy(k).wait_recv()
            here = pl.ds(start_of(k, 5) % 16, 2)
            n_sum[k, here] = n_sum[k, here] + n_recv2[k, 12:14]
            n_rs6_copy(k).start()
        phase("rs6")
        for side in range(2):
            base_copy(side).wait_recv()
        for k in portions:
            n_rs6_copy(k).wait_recv()
            place = start_of(k, 5) % 16
            mine_at = mine[k]["zc"]
            for i in range(2):
                summed = n_sum[k, place + i].astype(F32) + n_recv2[k, 14 + i].astype(F32)
                n_w[k, place + i] = (
                    anchor[(i + mine_at) % 2, k] - (outer_rate * (1.0 + outer_beta) * inner_rate * 0.25) * summed
                ).astype(BF16)
            n_ag5_copy(k).start()
        phase("outer")
        for k in portions:
            place = start_of(k, 6) % 16
            summed = n_sum[k, place].astype(F32) + n_recv2[k, 14 + mine[k]["zc"]].astype(F32)
            for s in range(SUBS):
                ch, tile = tile_of(k, s)
                rows = slice(tile * 8, tile * 8 + 8)
                lanes = slice(ch * 128, ch * 128 + 128)
                for c in range(2):
                    og[x_hi, c, rows, lanes] = (
                        og[x_hi, c, rows, lanes] + (inner_rate * 0.25) * summed[c, s * 8 : s * 8 + 8]
                    )
        for i in range(3):
            og_copy(i).start()
        phase("ag5")
        for k in portions:
            n_ag5_copy(k).wait_recv()
            for i in range(3):
                n_ag4_copy(k, i).start()
        phase("ag34")
        for k in portions:
            for i in range(3):
                n_ag4_copy(k, i).wait_recv()
            own_copy(k).start()
            for s in range(SUBS):
                for c in range(2):
                    a2_copy(k, s, c).start()
        for k in portions:
            weights[k, pl.ds(start_of(k, 2), 16)] = n_w[k, :, 1]

    @pl.when(core == 0)
    def _():
        phase("agown")
        for load in loads[8:10]:
            load.wait()
        for k in portions:
            own_copy(k).wait_recv()

    def ag_copy(k, j, s):
        here = pl.ds(start_of(k, j), 2 ** (6 - j))
        return remote(
            weights.at[k, here, rows_of(s)],
            weights.at[k, here, rows_of(s)],
            ag_send.at[k, j, s],
            ag_recv.at[k, j, s],
            partner(k, j, core),
        )

    for s in range(SUBS):
        phase(f"ag2{s}")
        for k in portions:
            a2_copy(k, s, 0).wait_recv()
            ag_copy(k, 1, s).start()
    for s in range(SUBS):
        phase(f"ag1{s}")
        for k in portions:
            ag_copy(k, 1, s).wait_recv()
            ag_copy(k, 0, s).start()

    def o_copy(ch):
        return remote(o_send.at[ch], o_recv.at[ch], o_ssem.at[ch], o_rsem.at[ch], sibling)

    def project():
        halves = [
            jnp.dot(
                ni[:, :, part * 2304 : part * 2304 + 2304].reshape(2 * SEQ, 2304),
                w_full[2 * part : 2 * part + 2].reshape(2304, 256),
                preferred_element_type=F32,
            )
            for part in range(2)
        ]
        return (halves[0] + halves[1]).astype(BF16)

    def to_output(half, ch, block):
        for t_hi in range(2):
            lanes = pl.ds(pl.multiple_of(half * 512 + t_hi * 256 + ch * 128, 128), 128)
            nk_ref[:, lanes] = block[:, t_hi * 128 : t_hi * 128 + 128]

    for ch in range(2):
        phase(f"ag0{ch}")
        for s in range(SUBS):
            for k in portions:
                if tile_of(k, s)[0] == ch:
                    ag_copy(k, 0, s).wait_recv()

        phase(f"place{ch}")
        def place_rows(c, _, ch=ch):
            for i in range(16):
                for t_hi in range(2):
                    for k in portions:
                        place = place_of(bits_of(k, t_hi, c // 2, c % 2, i // 4, i % 4), k)
                        for s in range(SUBS):
                            if tile_of(k, s)[0] == ch:
                                row = i * SHARD + tile_of(k, s)[1] * 8
                                w_full[c, row : row + 8, t_hi * 128 : t_hi * 128 + 128] = weights[
                                    k, place, s * 8 : s * 8 + 8
                                ]
            return 0

        lax.fori_loop(0, 4, place_rows, 0)
        if ch == 0:
            loads[10].wait()
            ni_copy.wait_recv()
        phase(f"proj{ch}")
        block = project()
        o_send[ch] = block[SEQ:]
        o_copy(ch).start()
        to_output(core, ch, block[:SEQ])

    phase("tail")
    @pl.when(core == 0)
    def _():
        og_copy(0).wait_recv()

    og_copy(1).wait_recv()
    for b in range(4):
        lanes = slice(b * 256, b * 256 + 256)
        outer = og[b % 2, b // 2]
        fresh = outer_beta * om_ref[:, lanes] + outer
        nm_ref[:, lanes] = fresh
        np_ref[:, lanes] = gp_ref[:, lanes] - outer_rate * (outer + outer_beta * fresh)
    phase("owait")
    for ch in range(2):
        o_copy(ch).wait_recv()
        to_output(1 - core, ch, o_recv[ch])

    phase("sends")
    for s in range(SUBS):
        for k in portions:
            for j in range(2):
                rs_copy(k, j, s).wait_send()
                ag_copy(k, j, s).wait_send()
            r2_copy(k, s, 0).wait_send()
    for ch in range(2):
        kg_copy(ch).wait_send()
        o_copy(ch).wait_send()
    xt_copy.wait_send()
    ni_copy.wait_send()
    for c in range(2):
        rep_copy(1, c, 0).wait_send()

    @pl.when(core == 0)
    def _():
        for c in range(2):
            rep_copy(0, c, 0).wait_send()
        for k in portions:
            for s in range(SUBS):
                keep_copy(k, s).wait_send()

    @pl.when(core == 1)
    def _():
        for i in range(3):
            og_copy(i).wait_send()
        for side in range(2):
            base_copy(side).wait_send()
        for k in portions:
            own_copy(k).wait_send()
            for i in range(3):
                n_rs4_copy(k, i).wait_send()
                n_ag4_copy(k, i).wait_send()
            n_rs5_copy(k).wait_send()
            n_rs6_copy(k).wait_send()
            n_ag5_copy(k).wait_send()
            for s in range(SUBS):
                for c in range(2):
                    a2_copy(k, s, c).wait_send()
    stack.close()


def store(np_ref, nm_ref, nk_ref, np_hbm, nm_hbm, nk_hbm, sems):
    copies = [
        pltpu.make_async_copy(src, dst, sems.at[i])
        for i, (src, dst) in enumerate(((nk_ref, nk_hbm), (np_ref, np_hbm), (nm_ref, nm_hbm)))
    ]
    for copy in copies:
        copy.start()
    for copy in copies:
        copy.wait()


def turning():
    half = HD // 2
    freqs = np.float32(rope_base) ** (-np.arange(half, dtype=np.float32) / np.float32(half))
    angles = np.arange(SEQ, dtype=np.float32)[:, None] * freqs[None, :].astype(np.float32)
    cosine, sine = np.cos(angles), np.sin(angles)
    return (
        np.concatenate([cosine, cosine], axis=1).astype(np.float32),
        np.concatenate([sine, -sine], axis=1).astype(np.float32),
    )


def body(layer_inputs, queries, saved_keys, saved_values, out_grad, global_params, replica_params, outer_momentum, next_inputs):
    cosine, sine = turning()
    vmem = pl.BlockSpec(memory_space=pltpu.VMEM)
    dma = pltpu.SemaphoreType.DMA
    rows = pltpu.VMEM((SHARD, 1024), F32)
    table = pltpu.VMEM((SEQ, HD), F32)
    results = pl.pallas_call(
        kernel,
        out_shape=(
            pltpu.VMEM((SHARD, 1024), F32),
            pltpu.VMEM((SHARD, 1024), F32),
            pltpu.VMEM((SEQ, 1024), BF16),
        ),
        in_specs=[pl.BlockSpec(memory_space=pltpu.HBM)] * 11,
        out_specs=(vmem, vmem, vmem),
        scratch_shapes=[
            pltpu.VMEM((SEQ, D), BF16),
            pltpu.VMEM((SEQ, 2048), BF16),
            pltpu.VMEM((SEQ, 1024), BF16),
            pltpu.VMEM((SEQ, 1024), BF16),
            pltpu.VMEM((SEQ, 2048), BF16),
            rows, rows, rows, table, table,
            pltpu.VMEM((2, SEQ, D), BF16),
            pltpu.VMEM((D, 512), BF16),
            pltpu.VMEM((2, 2, SEQ, 256), BF16),
            pltpu.VMEM((2, SEQ, 256), BF16),
            pltpu.VMEM((PORTIONS, 128, 24, 128), BF16),
            pltpu.VMEM((PORTIONS, 96, 24, 128), BF16),
            pltpu.VMEM((PORTIONS, 16, 24, 128), BF16),
            pltpu.VMEM((PORTIONS, 2, 16, 24, 128), BF16),
            pltpu.VMEM((PORTIONS, 16, 2, 24, 128), BF16),
            pltpu.VMEM((PORTIONS, 16, 2, 24, 128), BF16),
            pltpu.VMEM((PORTIONS, 16, 2, 24, 128), BF16),
            pltpu.VMEM((PORTIONS, 128, 24, 128), BF16),
            pltpu.VMEM((4, 1152, 256), BF16),
            pltpu.VMEM((3, 2, SHARD, 256), F32),
            pltpu.VMEM((2, 2, SHARD, 256), F32),
            pltpu.VMEM((2, SEQ, 256), BF16),
            pltpu.VMEM((2, SEQ, 256), BF16),
            pltpu.VMEM((2, PORTIONS, 2, 24, 128), F32),
            dma((11,)),
            dma((PORTIONS, 2, SUBS)), dma((PORTIONS, 2, SUBS)),
            dma((PORTIONS, SUBS)), dma((2, PORTIONS, SUBS)),
            dma((PORTIONS, SUBS)), dma((PORTIONS, SUBS)),
            dma((PORTIONS, 5)), dma((PORTIONS, 5)),
            dma((PORTIONS, 4)), dma((PORTIONS, 4)),
            dma((2, PORTIONS, SUBS)), dma((PORTIONS, SUBS)),
            dma((PORTIONS,)), dma((PORTIONS,)),
            dma((PORTIONS, 2, SUBS)), dma((PORTIONS, 2, SUBS)),
            dma((2, 2)), dma((3, 2)),
            dma((3,)), dma((2,)), dma((2,)), dma((2,)),
            dma, dma, dma, dma, dma((2,)), dma((2,)), dma((2,)), dma((2,)),
        ],
        compiler_params=pltpu.CompilerParams(
            collective_id=0, has_side_effects=True, vmem_limit_bytes=54 * 1024 * 1024
        ),
    )(
        layer_inputs, queries, saved_keys, saved_values, out_grad, global_params, replica_params[0],
        outer_momentum, cosine, sine, next_inputs,
    )
    return pl.pallas_call(
        store,
        out_shape=(
            jax.ShapeDtypeStruct((SHARD, 1024), F32),
            jax.ShapeDtypeStruct((SHARD, 1024), F32),
            jax.ShapeDtypeStruct((SEQ, 1024), BF16),
        ),
        in_specs=(vmem, vmem, vmem),
        out_specs=[pl.BlockSpec(memory_space=pltpu.HBM)] * 3,
        scratch_shapes=[dma((3,))],
        compiler_params=pltpu.CompilerParams(vmem_limit_bytes=4 * 1024 * 1024),
    )(*results)


def solution(mesh):
    both = ("rep", "fsdp")
    return jax.shard_map(
        body,
        mesh=mesh,
        in_specs=(
            P(both, None), P(both, None), P(both, None), P(both, None), P(both, None),
            P("fsdp", None), P("rep", "fsdp", None), P("fsdp", None), P(both, None),
        ),
        out_specs=(P("fsdp", None), P("fsdp", None), P(both, None)),
        check_vma=False,
    )
```
